32 devices in a mesh: seq: 8 (over z, core), tok: 4 (over y, x).
Axes of the slice: x: 2, y: 2, z: 4, core: 2. Of those that a mesh axis runs over, the one named last changes fastest.
Arguments:
- cotangent: bfloat16 [8, 512, 2048], P('seq', 'tok'), may hold values from -6 to 6
- gate_values: bfloat16 [8, 512, 2048], P('seq', 'tok'), may hold values from -6 to 6
- conv_input: bfloat16 [8, 512, 2048], P('seq', 'tok'), may hold values from -6 to 6
- filter_taps: float32 [2048, 512], P('tok', 'seq'), may hold values from -0.25 to 0.25
- first_moment: float32 [2048, 512], P('tok', 'seq'), may hold values from -12 to 12
- second_moment: float32 [2048, 512], P('tok', 'seq'), may hold values from 0.1 to 2
Outputs:
- grad_input: bfloat16 [8, 512, 2048], P('seq', 'tok')
- new_taps: float32 [2048, 512], P('tok', 'seq')
- new_first: float32 [2048, 512], P('tok', 'seq')
- new_second: float32 [2048, 512], P('tok', 'seq')
The draws below stay inside these ranges and needn't reach their ends.
All inputs are finite; a program needn't handle non-finite values.
Results may differ from the reference program's by a relative error of at most 0.0049.
Values may be sent and summed in bfloat16 or wider, within the bound.
No kernel may reach another device: no remote copies, remote signals or barrier semaphores. Data moves between devices by JAX's collectives and lax.ppermute only.
A program may use at most 64 MiB of HBM per device.

```python
import math
import jax
import jax.numpy as jnp
from jax import lax

D = 2048
LENGTH = 512
SEQS = 8


def block_levels(key, extent, pieces, least, largest):
    loudness, own = 1.0, jax.random.fold_in(key, 6)
    for position, blocks in pieces:
        heights = jnp.exp(jax.random.uniform(jax.random.fold_in(own, position), (blocks,), jnp.float32, least / len(pieces), largest / len(pieces)))
        loudness = loudness * jnp.repeat(heights, extent[position] // blocks).reshape([-1 if axis == position else 1 for axis in range(len(extent))])
    return loudness


def centred(stream_key, dims, width, reach, pieces=(), dtype=jnp.bfloat16):
    level = block_levels(stream_key, dims, pieces, -0.22, 0.18) if pieces else 1.0
    values = jax.random.normal(stream_key, dims, jnp.float32) * width * level
    return jnp.minimum(jnp.maximum(values, -reach), reach).astype(dtype)


def setup_inputs(seed: int = 0) -> dict:
    key_of = jax.random.split(jax.random.key(seed), 7)
    return {
        "cotangent": centred(key_of[0], (SEQS, LENGTH, D), 1.0, 6.0, ((0, 8), (1, 4))),
        "gate_values": centred(key_of[1], (SEQS, LENGTH, D), 1.0, 6.0, ((0, 8), (1, 4))),
        "conv_input": centred(key_of[2], (SEQS, LENGTH, D), 1.0, 6.0, ((0, 8), (1, 4))),
        "filter_taps": centred(key_of[3], (D, LENGTH), LENGTH ** -0.5, 0.25, ((0, 4), (1, 8)), jnp.float32),
        "first_moment": centred(key_of[4], (D, LENGTH), 3.0, 12.0, ((0, 4), (1, 8)), jnp.float32),
        "second_moment": jnp.clip(jnp.exp(math.log(2.0) - 2.9957323 * jax.random.uniform(key_of[5], (D, LENGTH), jnp.float32) ** block_levels(key_of[5], (D, LENGTH), ((0, 4), (1, 8)), -0.2, 0.2)), 0.1, 2.0),
    }


beta_one = 0.9
beta_two = 0.999
learn_rate = 0.05
adam_step = 10
adam_eps = 1e-08

def reference(cotangent, gate_values, conv_input, filter_taps, first_moment, second_moment):
    length = conv_input.shape[1]
    total_size = 2 * length
    spec_taps = jnp.fft.rfft(filter_taps.T, n=total_size, axis=0)

    def one_sequence(running, inputs_now):
        tangent, gate_now, source = inputs_now
        spec_source = jnp.fft.rfft(source.astype(jnp.float32), n=total_size, axis=0)
        scaled = lax.optimization_barrier((tangent.astype(jnp.float32) * gate_now.astype(jnp.float32)).astype(jnp.bfloat16)).astype(jnp.float32)
        spec_scaled = jnp.fft.rfft(scaled, n=total_size, axis=0)
        grad_input = jnp.fft.irfft(jnp.conj(spec_taps) * spec_scaled, n=total_size, axis=0)[:length].astype(jnp.bfloat16)
        taps_part = jnp.fft.irfft(jnp.conj(spec_source) * spec_scaled, n=total_size, axis=0)[:length]
        return (running + taps_part, grad_input)
    initial = jnp.zeros((length, filter_taps.shape[0]), jnp.float32)
    summed, grad_input = lax.scan(one_sequence, initial, (cotangent, gate_values, conv_input))
    taps_grad = summed.T / SEQS
    new_first = beta_one * first_moment + (1.0 - beta_one) * taps_grad
    new_second = beta_two * second_moment + (1.0 - beta_two) * taps_grad * taps_grad
    first_hat = new_first / (1.0 - beta_one ** adam_step)
    second_hat = new_second / (1.0 - beta_two ** adam_step)
    new_taps = filter_taps - learn_rate * first_hat / (jnp.sqrt(second_hat) + adam_eps)
    return (grad_input, new_taps, new_first, new_second)
```

```python
import math

import jax
import jax.numpy as jnp
import numpy as np
from jax import lax
from jax.experimental import pallas as pl
from jax.experimental.pallas import tpu as pltpu
from jax.sharding import PartitionSpec as P

beta_one = 0.9
beta_two = 0.999
learn_rate = 0.05
adam_step = 10
adam_eps = 1e-08

TABLE_BUDGET = 8 << 20


def inner_length(length):
    best_size = 1
    for candidate in range(1, math.isqrt(length) + 1):
        if length % candidate == 0:
            best_size = candidate
    return best_size


def angle_table(row_count, column_count, period):
    row_index = jnp.arange(row_count, dtype=jnp.int32)
    column_index = jnp.arange(column_count, dtype=jnp.int32)
    angles = (row_index[:, None] * column_index[None, :] % period).astype(jnp.float32) * (
        2.0 * math.pi / period
    )
    return (jnp.cos(angles), jnp.sin(angles))


def build_tables(length):
    inner_size = inner_length(length)
    half_rows = length // inner_size
    total_size = 2 * length
    cos_outer, sin_outer = angle_table(half_rows + 1, half_rows, 2 * half_rows)
    cos_inner, sin_inner = angle_table(inner_size, inner_size, inner_size)
    cos_twist, sin_twist = angle_table(half_rows + 1, inner_size, total_size)
    freq_index = jnp.arange(half_rows + 1, dtype=jnp.int32)
    weights = (
        jnp.where(jnp.logical_or(freq_index == 0, freq_index == half_rows), 1.0, 2.0).astype(
            jnp.float32
        )
        / total_size
    )
    back_cos = cos_outer.T * weights[None, :]
    back_sin = sin_outer.T * weights[None, :]
    return (
        (cos_outer, sin_outer),
        (cos_inner, sin_inner),
        (cos_twist[:, :, None], sin_twist[:, :, None]),
        (back_cos, back_sin),
    )


def contract(pattern, matrix, operand):
    return jnp.einsum(pattern, matrix, operand, precision=lax.Precision.HIGHEST)


def finish_forward(first_re, first_im, tables):
    cos_inner, sin_inner = tables[1]
    cos_twist, sin_twist = tables[2]
    turned_re = first_re * cos_twist + first_im * sin_twist
    turned_im = first_im * cos_twist - first_re * sin_twist
    paired = jnp.stack([cos_inner, sin_inner])
    from_real = contract("smq,kqc->skmc", paired, turned_re)
    from_imag = contract("smq,kqc->skmc", paired, turned_im)
    spec_re = from_real[0] + from_imag[1]
    spec_im = from_imag[0] - from_real[1]
    return (spec_re, spec_im)


def forward_time(signal, tables):
    cos_outer, sin_outer = tables[0]
    inner_size = tables[1][0].shape[0]
    operand = signal.reshape(signal.shape[0] // inner_size, inner_size, signal.shape[1])
    first = contract("skn,nqc->skqc", jnp.stack([cos_outer, -sin_outer]), operand)
    return finish_forward(first[0], first[1], tables)


def forward_channels(signal, tables):
    cos_outer, sin_outer = tables[0]
    inner_size = tables[1][0].shape[0]
    operand = signal.reshape(signal.shape[0], signal.shape[1] // inner_size, inner_size)
    first = contract("skn,cnq->skqc", jnp.stack([cos_outer, -sin_outer]), operand)
    return finish_forward(first[0], first[1], tables)


def conj_product(left_spec, right_spec):
    left_re, left_im = left_spec
    right_re, right_im = right_spec
    return (left_re * right_re + left_im * right_im, left_re * right_im - left_im * right_re)


def twisted_back(spectrum, tables):
    cos_inner, sin_inner = tables[1]
    cos_twist, sin_twist = tables[2]
    spec_re, spec_im = spectrum
    paired = jnp.stack([cos_inner, sin_inner])
    from_real = contract("sqm,kmc->skqc", paired, spec_re)
    from_imag = contract("sqm,kmc->skqc", paired, spec_im)
    back_re = from_real[0] - from_imag[1]
    back_im = from_imag[0] + from_real[1]
    turned_re = back_re * cos_twist - back_im * sin_twist
    turned_im = back_im * cos_twist + back_re * sin_twist
    return (turned_re, turned_im)


def time_rows(twisted, back_cos, back_sin):
    turned_re, turned_im = twisted
    signal = contract("nk,kqc->nqc", back_cos, turned_re) - contract(
        "nk,kqc->nqc", back_sin, turned_im
    )
    return signal.reshape(signal.shape[0] * signal.shape[1], signal.shape[2])


def factored_shards(cotangent, gate_values, conv_input, filter_taps, first_moment, second_moment):
    full_taps = lax.all_gather(filter_taps, "seq", axis=1, tiled=True)
    length = full_taps.shape[1]
    tables = build_tables(length)
    back_cos, back_sin = tables[3]
    scaled = (cotangent[0].astype(jnp.float32) * gate_values[0].astype(jnp.float32)).astype(
        jnp.bfloat16
    )
    scaled_chan, source_chan = (
        lax.all_to_all(scaled, "tok", split_axis=1, concat_axis=0, tiled=True),
        lax.all_to_all(conv_input[0], "tok", split_axis=1, concat_axis=0, tiled=True),
    )
    spec_taps = forward_channels(full_taps, tables)
    spec_source = forward_time(source_chan.astype(jnp.float32), tables)
    spec_scaled = forward_time(scaled_chan.astype(jnp.float32), tables)
    input_twisted = twisted_back(conj_product(spec_taps, spec_scaled), tables)
    input_grad = time_rows(input_twisted, back_cos, back_sin).astype(jnp.bfloat16)
    grad_input = lax.all_to_all(input_grad, "tok", split_axis=0, concat_axis=1, tiled=True)
    taps_twisted = twisted_back(conj_product(spec_source, spec_scaled), tables)
    summed = lax.psum_scatter(
        time_rows(taps_twisted, back_cos, back_sin).astype(jnp.bfloat16),
        "seq",
        scatter_dimension=0,
        tiled=True,
    ).astype(jnp.float32)
    taps_grad = summed.T / lax.axis_size("seq")
    new_first = beta_one * first_moment + (1.0 - beta_one) * taps_grad
    new_second = beta_two * second_moment + (1.0 - beta_two) * taps_grad * taps_grad
    first_hat = new_first / (1.0 - beta_one**adam_step)
    second_hat = new_second / (1.0 - beta_two**adam_step)
    new_taps = filter_taps - learn_rate * first_hat / (jnp.sqrt(second_hat) + adam_eps)
    return (grad_input[None], new_taps, new_first, new_second)


def call(body, out_shape, scratch=(), limit=40 << 20):
    return pl.pallas_call(
        body,
        out_shape=out_shape,
        scratch_shapes=list(scratch),
        compiler_params=pltpu.CompilerParams(vmem_limit_bytes=limit),
        name=body.__name__,
    )


def shape(dims, dtype):
    return jax.ShapeDtypeStruct(dims, dtype)


def mm(left, right):
    return jnp.dot(left, right, preferred_element_type=jnp.float32)


def angle_seeds(length):
    step = 1
    while step * step < length:
        step *= 2
    period = 2 * length
    column = np.arange(length)
    coarse = (np.arange(length // step) * step)[:, None] * column[None, :] % period
    fine = np.arange(step)[:, None] * column[None, :] % period
    unit = 2.0 * math.pi / period
    return [
        jnp.asarray(fn(part * unit), jnp.float32) for part in (coarse, fine) for fn in (np.cos, np.sin)
    ]


def dense_fits(length, n_tok, n_seq, channels):
    def power(n):
        return n & (n - 1) == 0

    tables = 6 * length * length * 2
    return (
        tables <= TABLE_BUDGET
        and power(n_tok)
        and power(n_seq)
        and power(length)
        and n_seq >= 2
        and (length // n_tok) % 16 == 0
        and (length // n_seq) % 16 == 0
        and channels % 128 == 0
    )


def make_dense(length, n_tok, n_seq, channels):
    tokens = length // n_tok
    lags = length // n_seq
    halves = n_seq // 2
    bf16, f32 = jnp.bfloat16, jnp.float32

    def split_store(value, high_ref, low_ref, rows):
        high = value.astype(bf16)
        high_ref[rows, :] = high
        low_ref[rows, :] = (value - high.astype(f32)).astype(bf16)

    def tables(cos_a, sin_a, cos_b, sin_b, ch, cl, sh, sl, th, tl):
        step = cos_b.shape[0]
        column = lax.broadcasted_iota(jnp.int32, (step, length), 1)
        row = lax.broadcasted_iota(jnp.int32, (step, length), 0)
        col_sign = jnp.where(column % 2 == 0, 1.0, -1.0).astype(f32)
        row_sign = jnp.where(row % 2 == 0, 1.0, -1.0).astype(f32)
        cos_fine, sin_fine = cos_b[...], sin_b[...]
        for block in range(length // step):
            ca, sa = cos_a[block : block + 1, :], sin_a[block : block + 1, :]
            rows = pl.ds(block * step, step)
            cosine = ca * cos_fine - sa * sin_fine
            sine = sa * cos_fine + ca * sin_fine
            split_store(cosine, ch, cl, rows)
            split_store(jnp.where(row + block * step == 0, col_sign, sine), sh, sl, rows)
            split_store(jnp.where(column == 0, row_sign, sine), th, tl, rows)

    def prep(cot, gate, src, *outs):
        mine = lax.axis_index("tok")
        for k in range(n_tok):
            start = pl.multiple_of((mine ^ k) * channels, channels)
            cols = pl.ds(start, channels)
            outs[k][0:tokens, :] = (
                cot[0, :, cols].astype(f32) * gate[0, :, cols].astype(f32)
            ).astype(bf16)
            outs[k][tokens : 2 * tokens, :] = src[0, :, cols]

    def taps_turn(taps, out):
        out[...] = taps[...].T.astype(bf16)

    def spectrum(ch, cl, sh, sl, value):
        return mm(ch, value) + mm(cl, value), mm(sh, value) + mm(sl, value)

    def taps_forward(*refs):
        own, others = refs[0:halves], refs[halves]
        ch, cl, sh, sl, re_out, im_out, full = refs[halves + 1 :]
        mine = lax.axis_index("seq")
        for j in range(halves):
            full[pl.ds(pl.multiple_of((mine ^ (2 * j)) * lags, lags), lags), :] = own[j][...]
            full[pl.ds(pl.multiple_of((mine ^ (2 * j + 1)) * lags, lags), lags), :] = others[
                pl.ds(j * lags, lags), :
            ]
        re, im = spectrum(ch[...], cl[...], sh[...], sl[...], full[...])
        re_out[...] = re
        im_out[...] = im

    def product(left_re, left_im, right_re, right_im):
        first = lax.broadcasted_iota(jnp.int32, left_re.shape, 0) == 0
        edge = 1.0 / (2 * length)
        cross_re, cross_im = left_re * right_re, left_im * right_im
        out_re = jnp.where(first, cross_re * edge, (cross_re + cross_im) * (2.0 * edge))
        out_im = jnp.where(
            first, cross_im * edge, (left_re * right_im - left_im * right_re) * (2.0 * edge)
        )
        return out_re, out_im

    def main_taps(*refs):
        pieces = refs[0:n_tok]
        ch, cl, sh, sl, th, tl = refs[n_tok : n_tok + 6]
        keep, send, re_out, im_out, scaled, source, grad = refs[n_tok + 6 :]
        mine = lax.axis_index("tok")
        for k in range(n_tok):
            rows = pl.ds(pl.multiple_of((mine ^ k) * tokens, tokens), tokens)
            scaled[rows, :] = pieces[k][0:tokens, :]
            source[rows, :] = pieces[k][tokens : 2 * tokens, :]
        scaled_re, scaled_im = spectrum(ch[...], cl[...], sh[...], sl[...], scaled[...])
        re_out[...] = scaled_re
        im_out[...] = scaled_im
        source_re, source_im = spectrum(ch[...], cl[...], sh[...], sl[...], source[...])
        prod_re, prod_im = product(source_re, source_im, scaled_re, scaled_im)
        prod_re, prod_im = prod_re.astype(bf16), prod_im.astype(bf16)
        grad[...] = (
            mm(ch[...], prod_re) + mm(cl[...], prod_re) + mm(th[...], prod_im) + mm(tl[...], prod_im)
        )
        place = lax.axis_index("seq")
        for j in range(halves):
            here = pl.ds(pl.multiple_of((place ^ (2 * j)) * lags, lags), lags)
            there = pl.ds(pl.multiple_of((place ^ (2 * j + 1)) * lags, lags), lags)
            keep[pl.ds(j * lags, lags), :] = grad[here, :]
            send[pl.ds(j * lags, lags), :] = grad[there, :].astype(bf16)

    def main_input(*refs):
        taps_re, taps_im, scaled_re, scaled_im, ch, cl, th, tl = refs[0:8]
        outs, grad = refs[8 : 8 + n_tok], refs[8 + n_tok]
        prod_re, prod_im = product(taps_re[...], taps_im[...], scaled_re[...], scaled_im[...])
        high_re, high_im = prod_re.astype(bf16), prod_im.astype(bf16)
        low_re = (prod_re - high_re.astype(f32)).astype(bf16)
        low_im = (prod_im - high_im.astype(f32)).astype(bf16)
        grad[...] = (
            mm(ch[...], high_re)
            + mm(cl[...], high_re)
            + mm(ch[...], low_re)
            + mm(th[...], high_im)
            + mm(tl[...], high_im)
            + mm(th[...], low_im)
        )
        mine = lax.axis_index("tok")
        for k in range(n_tok):
            rows = pl.ds(pl.multiple_of((mine ^ k) * tokens, tokens), tokens)
            outs[k][...] = grad[rows, :].astype(bf16)

    def pair_sum(*refs):
        keep, got, own = refs[0:3]
        sends = refs[3:]
        for j in range(halves):
            rows = pl.ds(j * lags, lags)
            total = keep[rows, :] + got[rows, :].astype(f32)
            if j == 0:
                own[...] = total
            else:
                sends[j - 1][...] = total.astype(bf16)

    def assemble(*refs):
        pieces, out = refs[0:n_tok], refs[n_tok]
        mine = lax.axis_index("tok")
        for k in range(n_tok):
            start = pl.multiple_of((mine ^ k) * channels, channels)
            out[0, :, pl.ds(start, channels)] = pieces[k][...]

    def adam(*refs):
        own = refs[0]
        others = refs[1:halves]
        taps, first, second, new_taps, new_first, new_second = refs[halves:]
        total = own[...]
        for other in others:
            total = total + other[...].astype(f32)
        grad = total.T / n_seq
        moment_one = beta_one * first[...] + (1.0 - beta_one) * grad
        moment_two = beta_two * second[...] + (1.0 - beta_two) * grad * grad
        new_first[...] = moment_one
        new_second[...] = moment_two
        first_hat = moment_one / (1.0 - beta_one**adam_step)
        second_hat = moment_two / (1.0 - beta_two**adam_step)
        new_taps[...] = taps[...] - learn_rate * first_hat / (jnp.sqrt(second_hat) + adam_eps)

    tok_pairs = [[(i, i ^ k) for i in range(n_tok)] for k in range(n_tok)]
    seq_pairs = [[(i, i ^ k) for i in range(n_seq)] for k in range(n_seq)]
    table_shape = shape((length, length), bf16)
    wide = shape((length, channels), f32)

    def dense_shards(cotangent, gate_values, conv_input, filter_taps, first_moment, second_moment):
        sends = call(prep, [shape((2 * tokens, channels), bf16)] * n_tok)(
            cotangent, gate_values, conv_input
        )
        turned = call(taps_turn, shape((lags, channels), bf16))(filter_taps)
        pieces = [sends[0]] + [
            lax.ppermute(sends[k], "tok", tok_pairs[k]) for k in range(1, n_tok)
        ]
        taps_own = [turned] + [
            lax.ppermute(turned, "seq", seq_pairs[2 * j]) for j in range(1, halves)
        ]
        ch, cl, sh, sl, th, tl = call(tables, [table_shape] * 6)(*angle_seeds(length))
        taps_other = lax.ppermute(jnp.concatenate(taps_own, axis=0), "seq", seq_pairs[1])
        taps_re, taps_im = call(
            taps_forward, [wide, wide], [pltpu.VMEM((length, channels), bf16)]
        )(*taps_own, taps_other, ch, cl, sh, sl)
        keep, send, scaled_re, scaled_im = call(
            main_taps,
            [
                shape((halves * lags, channels), f32),
                shape((halves * lags, channels), bf16),
                wide,
                wide,
            ],
            [pltpu.VMEM((length, channels), bf16)] * 2 + [pltpu.VMEM((length, channels), f32)],
        )(*pieces, ch, cl, sh, sl, th, tl)
        got = lax.ppermute(send, "seq", seq_pairs[1])
        grads = call(
            main_input,
            [shape((tokens, channels), bf16)] * n_tok,
            [pltpu.VMEM((length, channels), f32)],
        )(taps_re, taps_im, scaled_re, scaled_im, ch, cl, th, tl)
        sums = call(
            pair_sum,
            [shape((lags, channels), f32)] + [shape((lags, channels), bf16)] * (halves - 1),
        )(keep, got)
        back = [grads[0]] + [lax.ppermute(grads[k], "tok", tok_pairs[k]) for k in range(1, n_tok)]
        partial = [sums[0]] + [
            lax.ppermute(sums[j], "seq", seq_pairs[2 * j]) for j in range(1, halves)
        ]
        grad_input = call(assemble, shape((1, tokens, n_tok * channels), bf16))(*back)
        out = shape((channels, lags), f32)
        new_taps, new_first, new_second = call(adam, [out, out, out])(
            *partial, filter_taps, first_moment, second_moment
        )
        return (grad_input, new_taps, new_first, new_second)

    return dense_shards


def shards(cotangent, gate_values, conv_input, filter_taps, first_moment, second_moment):
    n_tok, n_seq = lax.axis_size("tok"), lax.axis_size("seq")
    channels, lags = filter_taps.shape
    length = lags * n_seq
    if dense_fits(length, n_tok, n_seq, channels):
        body = make_dense(length, n_tok, n_seq, channels)
    else:
        body = factored_shards
    return body(cotangent, gate_values, conv_input, filter_taps, first_moment, second_moment)


def solution(mesh):
    placed = (
        P("seq", "tok", None),
        P("seq", "tok", None),
        P("seq", "tok", None),
        P("tok", "seq"),
        P("tok", "seq"),
        P("tok", "seq"),
    )
    return jax.shard_map(
        shards,
        mesh=mesh,
        in_specs=placed,
        out_specs=(P("seq", "tok", None), P("tok", "seq"), P("tok", "seq"), P("tok", "seq")),
        check_vma=False,
    )
```
